256 devices in a mesh: tok: 32 (over x, z), feat: 8 (over y, core).
Axes of the slice: x: 4, y: 4, z: 8, core: 2. Of those that a mesh axis runs over, the one named last changes fastest.
Arguments:
- slab: bfloat16 [65536, 8192], P('tok', 'feat'), may hold values from -48 to 48
- sketch: bfloat16 [8192, 512], P('feat'), may hold values from -0.0625 to 0.0625
Outputs:
- q_basis: bfloat16 [65536, 512], P('tok')
- r_scaled: float32 [512, 512], replicated
- projected: float32 [8192, 512], P(('feat', 'tok'))
The draws below stay inside these ranges and needn't reach their ends.
All inputs are finite; a program needn't handle non-finite values.
Results may differ from the reference program's by a relative error of at most 0.011.
Values may be sent and summed in bfloat16 or wider, within the bound.
No kernel may reach another device: no remote copies, remote signals or barrier semaphores. Data moves between devices by JAX's collectives and lax.ppermute only.
A program may use at most 64 MiB of HBM per device.

```python
import math
import jax
import jax.numpy as jnp
from jax import lax

D = 8192
K = 512
TOKENS = 65536


def draw_slab(key, part):
    directions = max(K // 8, 2)
    spread = 0.01
    subkeys = jax.random.split(jax.random.fold_in(key, 7), 3)
    factors = jax.random.normal(subkeys[1], (directions, D), jnp.float32) / math.sqrt(D)
    position = jnp.arange(TOKENS).astype(jnp.float32) / (TOKENS - 1)
    condition = 3.0
    loadings = jax.random.normal(subkeys[0], (TOKENS, directions), jnp.float32)
    jitter = jax.random.normal(subkeys[2], (TOKENS, D), jnp.float32)
    rise = 4.0
    profile = jnp.exp(-math.log(16.0) * jnp.arange(directions).astype(jnp.float32) / (directions - 1))
    leading = condition * spread * (1.0 - math.sqrt(K / TOKENS)) * math.sqrt(D / K)
    planted = jnp.dot(loadings * (leading * profile)[None, :], factors, precision=lax.Precision.HIGHEST, preferred_element_type=jnp.float32)
    row_scale = jnp.exp(math.log(rise) * (position - 0.5))
    result = jnp.clip((planted + spread * jitter) * row_scale[:, None], -48.0, 48.0)
    return result.astype(jnp.bfloat16)


def levels(key, extent, shards, least, high):
    level, own = 1.0, jax.random.fold_in(key, 6)
    for dim, shards_of in shards:
        heights = jnp.exp(jax.random.uniform(jax.random.fold_in(own, dim), (shards_of,), jnp.float32, least / len(shards), high / len(shards)))
        level = level * jnp.repeat(heights, extent[dim] // shards_of).reshape([-1 if axis == dim else 1 for axis in range(len(extent))])
    return level


def gaussian(key, dims, deviation, bound, cuts=(), dtype=jnp.bfloat16):
    drawn = jax.random.normal(key, dims, jnp.float32) * deviation
    if len(cuts) > 0:
        drawn = levels(key, dims, cuts, -0.22, 0.18) * drawn
    return jnp.clip(drawn, min=-bound, max=bound).astype(dtype)


def setup_inputs(seed: int = 0) -> dict:
    streams_of = jax.random.split(jax.random.key(seed), 3)
    slab = draw_slab(jax.random.fold_in(streams_of[2], 71), 0)
    sketch = gaussian(streams_of[1], (D, K), D ** -0.5, 0.0625, ((0, 8),))
    return dict(slab=slab, sketch=sketch)


def reference(slab, sketch):
    sketched = jnp.dot(slab.astype(jnp.float32), sketch.astype(jnp.float32), preferred_element_type=jnp.float32)
    basis, factor = jnp.linalg.qr(sketched)
    signs = jnp.sign(jnp.diagonal(factor))
    basis = basis * signs[None, :]
    factor = factor * signs[:, None]
    q_basis = basis.astype(jnp.bfloat16)
    r_scaled = factor / jnp.sqrt(jnp.float32(TOKENS))
    projected = jnp.dot(slab.T.astype(jnp.float32), q_basis.astype(jnp.float32), preferred_element_type=jnp.float32)
    return (q_basis, r_scaled, projected)
```

```python
import jax
import jax.numpy as jnp
from jax import lax
from jax.experimental import pallas as pl
from jax.experimental.pallas import tpu as pltpu
from jax.sharding import Mesh
from jax.sharding import PartitionSpec as P

HIGH = lax.Precision.HIGHEST
NB, PB = 128, 8

def diag_factor(block):
    sub = lax.broadcasted_iota(jnp.int32, (PB, NB), 0)
    lane = lax.broadcasted_iota(jnp.int32, (PB, NB), 1)
    n = NB // PB
    xs = [block[PB * p:PB * (p + 1), :] for p in range(n)]
    vs = [jnp.where(lane == sub + PB * p, 1.0, 0.0).astype(jnp.float32) for p in range(n)]
    rows, invs = [], []
    for p in range(n):
        x, v = xs[p], vs[p]
        cols = [jnp.broadcast_to(x[:, PB * p + k:PB * p + k + 1], (PB, NB)) for k in range(PB)]
        scale = jnp.ones((PB, NB), jnp.float32)
        for k in range(PB):
            r = lax.rsqrt(jnp.broadcast_to(cols[k][k:k + 1, :], (PB, NB)))
            scale = jnp.where(sub == k, r, scale)
            coef = jnp.where(sub > k, cols[k] * (r * r), 0.0)
            for j in range(k + 1, PB):
                cols[j] = cols[j] - coef * cols[j][k:k + 1, :]
            x = x - coef * x[k:k + 1, :]
            v = v - coef * v[k:k + 1, :]
        x, v = x * scale, v * scale
        rows.append(jnp.where(lane >= sub + PB * p, x, 0.0))
        invs.append(v)
        for q in range(p + 1, n):
            pick = lane == sub + PB * q
            for k in range(PB):
                row = jnp.broadcast_to(x[k:k + 1, :], (PB, NB))
                c = jnp.sum(jnp.where(pick, row, 0.0), axis=1, keepdims=True)
                xs[q] = xs[q] - c * row
                vs[q] = vs[q] - c * v[k:k + 1, :]
    return jnp.concatenate(rows, 0), jnp.concatenate(invs, 0)

def tn(a, b):
    return lax.dot_general(a, b, (((0,), (0,)), ((), ())), precision=HIGH, preferred_element_type=jnp.float32)

def nn(a, b):
    return jnp.dot(a, b, precision=HIGH, preferred_element_type=jnp.float32)

def factor_in_place(s_ref, r_ref, w_ref):
    n = s_ref.shape[0] // NB
    at = lambda i: slice(NB * i, NB * (i + 1))
    r_ref[...] = jnp.zeros_like(r_ref)
    w_ref[...] = jnp.zeros_like(w_ref)
    for b in range(n):
        upper, inv = diag_factor(s_ref[at(b), at(b)])
        r_ref[at(b), at(b)] = upper
        w_ref[at(b), at(b)] = inv
        if b:
            left = tn(r_ref[0:NB * b, at(b)], w_ref[0:NB * b, 0:NB * b])
            w_ref[at(b), 0:NB * b] = -nn(inv, left)
        if b < n - 1:
            rest = slice(NB * (b + 1), NB * n)
            r_ref[at(b), rest] = nn(inv, s_ref[at(b), rest])
            for j in range(b + 1, n):
                tail = slice(NB * j, NB * n)
                s_ref[at(j), tail] = s_ref[at(j), tail] - tn(r_ref[at(b), at(j)], r_ref[at(b), tail])

X, Z, Y, C = "tok_0", "tok_1", "feat_0", "feat_1"
TOK = (X, Z)
LEVEL = 14.0
TAIL = 8
F32, BF16, F16 = jnp.float32, jnp.bfloat16, jnp.float16
VMEM = pl.BlockSpec(memory_space=pltpu.VMEM)
SMEM = pl.BlockSpec(memory_space=pltpu.SMEM)


def struct(shape, dtype):
    return jax.ShapeDtypeStruct(shape, dtype)


def exchange(blocks, axis):
    return lax.all_to_all(blocks, axis, 0, 0, tiled=True)


def sent_to_all(array, axis):
    peers = lax.axis_size(axis)
    return exchange(jnp.broadcast_to(array[None], (peers, *array.shape)), axis)


def from_partner(array):
    return lax.ppermute(array, C, [(0, 1), (1, 0)])


def packed(values):
    power = jnp.clip(jnp.floor(jnp.log2(jnp.max(jnp.abs(values)))), -100.0, 40.0)
    tail = jnp.full((*values.shape[:-2], TAIL, values.shape[-1]), power.astype(F16))
    return jnp.concatenate([(values * jnp.exp2(LEVEL - power)).astype(F16), tail], axis=-2)


def unpacked(blocks):
    rows = blocks.shape[1] - TAIL
    power = blocks[:, rows : rows + 1, :1].astype(F32)
    return blocks[:, :rows, :].astype(F32) * jnp.exp2(power - LEVEL)


def split(blocks):
    values = unpacked(blocks).reshape(-1, blocks.shape[-1])
    high = lax.reduce_precision(values, 8, 7)
    return high.astype(BF16), (values - high).astype(BF16)


def dot_tn(a, b):
    return lax.dot_general(a, b, (((0,), (0,)), ((), ())), preferred_element_type=F32)


def dot_nt(a, b):
    return lax.dot_general(a, b, (((1,), (1,)), ((), ())), preferred_element_type=F32)


def share_kernel(place_ref, high_ref, low_ref, share_ref):
    strip = share_ref.shape[0]
    at = pl.ds(pl.multiple_of(place_ref[1] * strip, strip), strip)
    high, low = high_ref[...], low_ref[...]
    share_ref[...] = dot_tn(high_ref[:, at], high) + (
        dot_tn(high_ref[:, at], low) + dot_tn(low_ref[:, at], high)
    )


def basis_kernel(
    place_ref, mine_ref, other_ref, hm_ref, lm_ref, ho_ref, lo_ref, q_ref, r_ref, w_ref, s_ref, wh_ref, wl_ref
):
    core = place_ref[0]
    blocks, half, columns = mine_ref.shape
    for i in range(blocks):
        s_ref[pl.ds(pl.multiple_of(2 * half * i + half * core, half), half), :] = mine_ref[i]
        s_ref[pl.ds(pl.multiple_of(2 * half * i + half * (1 - core), half), half), :] = other_ref[i]
    factor_in_place(s_ref, r_ref, w_ref)
    inverse = w_ref[...]
    high = inverse.astype(BF16)
    wh_ref[...] = high
    wl_ref[...] = (inverse - high.astype(F32)).astype(BF16)
    rows = hm_ref.shape[0]
    step = 256
    for place, h_ref, l_ref in ((core, hm_ref, lm_ref), (1 - core, ho_ref, lo_ref)):
        def some_rows(i, _, place=place, h_ref=h_ref, l_ref=l_ref):
            at = pl.ds(pl.multiple_of(i * step, step), step)
            out = pl.ds(pl.multiple_of(place * rows + i * step, step), step)
            for j in range(0, columns, 256):
                k = j + 256
                wh, wl = wh_ref[j:k, :k], wl_ref[j:k, :k]
                h = h_ref[at, :k]
                q_ref[out, j:k] = (
                    dot_nt(h, wh) + (dot_nt(h, wl) + dot_nt(l_ref[at, :k], wh))
                ).astype(BF16)
            return 0
        lax.fori_loop(0, rows // step, some_rows, 0)


def body(slab, sketch):
    core, row = lax.axis_index(C), lax.axis_index(Y)
    place = jnp.stack([core, row]).astype(jnp.int32)
    tokens, columns = slab.shape[0], sketch.shape[1]
    half, block, strip = tokens // 2, tokens // 8, columns // 4
    halves = slab.reshape(2, half, slab.shape[1])

    def half_rows(which):
        return lax.dynamic_index_in_dim(halves, which, 0, keepdims=False)

    def partial(which):
        return jnp.dot(half_rows(which), sketch, preferred_element_type=F32)

    theirs = from_partner(partial(1 - core))
    pair_sum = (partial(core) + theirs).reshape(4, block, columns)
    own = unpacked(exchange(packed(pair_sum), Y)).sum(axis=0)
    mine = sent_to_all(packed(own), Y)
    other = from_partner(mine)
    high_mine, low_mine = split(mine)
    share = pl.pallas_call(
        share_kernel,
        out_shape=struct((strip, columns), F32),
        in_specs=[SMEM, VMEM, VMEM],
        out_specs=VMEM,
        name="share",
    )(place, high_mine, low_mine)
    high_other, low_other = split(other)

    shares = share.reshape(2, strip // 2, columns)
    kept = lax.dynamic_index_in_dim(shares, core, 0, keepdims=False)
    given = lax.dynamic_index_in_dim(shares, 1 - core, 0, keepdims=False)
    strip_sum = kept + from_partner(given)
    total = exchange(strip_sum.reshape(32, -1, columns), TOK).sum(axis=0)
    done = sent_to_all(total, TOK).reshape(strip // 2, columns)

    def onto(which, values):
        return lax.dot_general(
            half_rows(which), values, (((0,), (0,)), ((), ())), preferred_element_type=F32
        )

    images = onto(core, high_mine) + onto(core, low_mine)
    images = images + (onto(1 - core, high_other) + onto(1 - core, low_other))
    image = exchange(images.astype(BF16).reshape(32, -1, columns), TOK)

    strips = sent_to_all(done, Y)
    square = struct((columns, columns), F32)
    q_basis, upper, inverse = pl.pallas_call(
        basis_kernel,
        out_shape=(struct((tokens, columns), BF16), square, square),
        in_specs=[SMEM] + [VMEM] * 6,
        out_specs=(VMEM,) * 3,
        scratch_shapes=[
            pltpu.VMEM((columns, columns), F32),
            pltpu.VMEM((columns, columns), BF16),
            pltpu.VMEM((columns, columns), BF16),
        ],
        name="basis",
    )(place, strips, from_partner(strips), high_mine, low_mine, high_other, low_other)
    token_count = tokens * lax.axis_size(TOK)
    r_scaled = upper / jnp.sqrt(jnp.float32(token_count))
    projected = lax.dot_general(
        image.astype(F32).sum(axis=0), inverse, (((1,), (1,)), ((), ())), precision=HIGH,
        preferred_element_type=F32,
    )
    return (q_basis, r_scaled, projected)


def solution(mesh):
    split_mesh = Mesh(mesh.devices.reshape(4, 8, 4, 2), (X, Z, Y, C))
    in_specs = (P(TOK, (Y, C)), P((Y, C), None))
    out_specs = (P(TOK, None), P(), P((Y, C, X, Z), None))
    return jax.shard_map(body, mesh=split_mesh, in_specs=in_specs, out_specs=out_specs, check_vma=False)
```

```python
import functools
import math

import jax
import jax.numpy as jnp
from jax import lax
from jax.experimental import pallas as pl
from jax.experimental.pallas import tpu as pltpu
from jax.sharding import Mesh
from jax.sharding import PartitionSpec as P

HIGH = lax.Precision.HIGHEST
NB, PB = 128, 8


def row_of(tile, k):
    return jnp.broadcast_to(tile[k : k + 1, :], (PB, NB))


def diag_factor(block):
    sub = lax.broadcasted_iota(jnp.int32, (PB, NB), 0)
    lane = lax.broadcasted_iota(jnp.int32, (PB, NB), 1)
    n = NB // PB
    xs = [block[PB * p : PB * (p + 1), :] for p in range(n)]
    vs = [jnp.where(lane == sub + PB * p, 1.0, 0.0).astype(jnp.float32) for p in range(n)]
    for p in range(0, n, 2):
        first = PB * p
        x, v = xs[p : p + 2], vs[p : p + 2]
        cols = [
            [jnp.broadcast_to(x[h][:, first + k : first + k + 1], (PB, NB)) for h in range(2)]
            for k in range(2 * PB)
        ]
        scale = [jnp.ones((PB, NB), jnp.float32)] * 2
        for k in range(2 * PB):
            h, i = divmod(k, PB)
            pivot = row_of(cols[k][h], i)
            below = {h: jnp.where(sub > i, cols[k][h], 0.0)}
            if h == 0:
                below[1] = cols[k][1]
            r = lax.rsqrt(pivot)
            square = r * r
            if k + 1 < 2 * PB:
                head = row_of(cols[k + 1][h], i)
                for g in below:
                    cols[k + 1][g] = cols[k + 1][g] - (below[g] * head) * square
            coef = {g: below[g] * square for g in below}
            scale[h] = jnp.where(sub == i, r, scale[h])
            for j in range(k + 2, 2 * PB):
                head = row_of(cols[j][h], i)
                for g in below:
                    cols[j][g] = cols[j][g] - coef[g] * head
            for m in (x, v):
                head = row_of(m[h], i)
                for g in below:
                    m[g] = m[g] - coef[g] * head
        for h in range(2):
            x[h], v[h] = x[h] * scale[h], v[h] * scale[h]
        xs[p : p + 2], vs[p : p + 2] = x, v
        for q in range(p + 2, n):
            pick = lane == sub + PB * q
            for k in range(2 * PB):
                h, i = divmod(k, PB)
                row = row_of(x[h], i)
                c = jnp.sum(jnp.where(pick, row, 0.0), axis=1, keepdims=True)
                xs[q] = xs[q] - c * row
                vs[q] = vs[q] - c * row_of(v[h], i)
    rows = [jnp.where(lane >= sub + PB * p, xs[p], 0.0) for p in range(n)]
    return jnp.concatenate(rows, 0), jnp.concatenate(vs, 0)


def tn(a, b):
    return lax.dot_general(
        a, b, (((0,), (0,)), ((), ())), precision=HIGH, preferred_element_type=jnp.float32
    )


def nn(a, b):
    return jnp.dot(a, b, precision=HIGH, preferred_element_type=jnp.float32)


def factor_in_place(s_ref, r_ref, w_ref):
    n = s_ref.shape[0] // NB

    def at(i):
        return slice(NB * i, NB * (i + 1))

    r_ref[...] = jnp.zeros_like(r_ref)
    w_ref[...] = jnp.zeros_like(w_ref)
    def factor_block(b, _):
        here = pl.ds(pl.multiple_of(b * NB, NB), NB)
        upper, inv = diag_factor(s_ref[here, here])
        r_ref[here, here] = upper
        w_ref[here, here] = inv
        for i in range(n):
            pl.when(b == i)(functools.partial(after_block, i))
        return 0

    def after_block(b):
        inv = w_ref[at(b), at(b)]
        if b < n - 1:
            rest = slice(NB * (b + 1), NB * n)
            r_ref[at(b), rest] = nn(inv, s_ref[at(b), rest])
            for j in range(b + 1, n):
                tail = slice(NB * j, NB * n)
                s_ref[at(j), tail] = s_ref[at(j), tail] - tn(r_ref[at(b), at(j)], r_ref[at(b), tail])
        if b:
            left = tn(r_ref[0 : NB * b, at(b)], w_ref[0 : NB * b, 0 : NB * b])
            w_ref[at(b), 0 : NB * b] = -nn(inv, left)

    lax.fori_loop(0, n, factor_block, 0)

X, Z, Y, C = "tok_0", "tok_1", "feat_0", "feat_1"
TOK = (X, Z)
LEVEL = 14.0
TAIL = 8
F32, BF16, F16 = jnp.float32, jnp.bfloat16, jnp.float16
VMEM = pl.BlockSpec(memory_space=pltpu.VMEM)
SMEM = pl.BlockSpec(memory_space=pltpu.SMEM)


def struct(shape, dtype):
    return jax.ShapeDtypeStruct(shape, dtype)


def exchange(blocks, axis):
    return lax.all_to_all(blocks, axis, 0, 0, tiled=True)


def shifted(array, axis, shift):
    peers = lax.axis_size(axis)
    return lax.ppermute(array, axis, [(i, (i + shift) % peers) for i in range(peers)])


def flipped(array, axis, bit):
    return lax.ppermute(array, axis, [(i, i ^ bit) for i in range(lax.axis_size(axis))])


def from_partner(array):
    return flipped(array, C, 1)


def block_of(blocks, i):
    return lax.dynamic_index_in_dim(blocks, i, 0, keepdims=False)


def packed(values, power):
    tail = jnp.full((TAIL, values.shape[1]), power.astype(F16))
    return jnp.concatenate([(values * jnp.exp2(LEVEL - power)).astype(F16), tail])


def unpacked(block):
    rows = block.shape[0] - TAIL
    power = block[rows, 0].astype(F32)
    return block[:rows].astype(F32) * jnp.exp2(power - LEVEL), power


def split(values):
    high = lax.reduce_precision(values, 8, 7)
    return high.astype(BF16), (values - high).astype(BF16)


def dot_tn(a, b):
    return lax.dot_general(a, b, (((0,), (0,)), ((), ())), preferred_element_type=F32)


def dot_nn(a, b):
    return jnp.dot(a, b, preferred_element_type=F32)


def part(i, size):
    return pl.ds(pl.multiple_of(i * size, size), size)


def share_kernel(place_ref, *refs):
    highs, lows = refs[0:4], refs[4:8]
    high_ref, low_ref, kept_ref, given_ref, strip_ref = refs[8:]
    core, row = place_ref[0], place_ref[1]
    block = highs[0].shape[0]
    for s in range(4):
        at = part(lax.rem(row + 4 - s, 4), block)
        high_ref[at, :] = highs[s][...]
        low_ref[at, :] = lows[s][...]
    strip, half = strip_ref.shape[0], kept_ref.shape[0]
    lanes = part(row, strip)
    high, low = high_ref[...], low_ref[...]
    strip_ref[...] = dot_tn(high_ref[:, lanes], high) + (
        dot_tn(high_ref[:, lanes], low) + dot_tn(low_ref[:, lanes], high)
    )
    kept_ref[...] = strip_ref[part(core, half), :]
    given_ref[...] = strip_ref[part(1 - core, half), :]


def basis_kernel(scale, place_ref, *refs):
    mine, other = refs[0:4], refs[4:8]
    hm_ref, lm_ref, ho_ref, lo_ref, q_ref, out_ref, uh_ref, ul_ref, s_ref, r_ref, w_ref = refs[8:]
    core, row = place_ref[0], place_ref[1]
    half = mine[0].shape[0]
    columns = s_ref.shape[0]
    for s in range(4):
        strip = 2 * lax.rem(row + 4 - s, 4)
        s_ref[part(strip + core, half), :] = mine[s][...]
        s_ref[part(strip + 1 - core, half), :] = other[s][...]
    factor_in_place(s_ref, r_ref, w_ref)
    out_ref[...] = r_ref[...] * scale
    for j in range(0, columns, NB):
        u = w_ref[j : j + NB, :].T
        high = u.astype(BF16)
        uh_ref[:, j : j + NB] = high
        ul_ref[:, j : j + NB] = (u - high.astype(F32)).astype(BF16)
    rows = hm_ref.shape[0]
    step = 256
    for place, h_ref, l_ref in ((core, hm_ref, lm_ref), (1 - core, ho_ref, lo_ref)):

        def some_rows(i, _, place=place, h_ref=h_ref, l_ref=l_ref):
            at, out = part(i, step), part(place * (rows // step) + i, step)
            for j in range(0, columns, 256):
                k = j + 256
                h, l = h_ref[at, :k], l_ref[at, :k]
                uh, ul = uh_ref[:k, j:k], ul_ref[:k, j:k]
                q_ref[out, j:k] = (dot_nn(h, uh) + (dot_nn(h, ul) + dot_nn(l, uh))).astype(BF16)
            return 0

        lax.fori_loop(0, rows // step, some_rows, 0)


def image_kernel(in_ref, uh_ref, ul_ref, out_ref):
    total = in_ref[0].astype(F32)
    for i in range(1, in_ref.shape[0]):
        total = total + in_ref[i].astype(F32)
    high = total.astype(BF16)
    low = (total - high.astype(F32)).astype(BF16)
    uh = uh_ref[...]
    out_ref[...] = dot_nn(high, uh) + (dot_nn(high, ul_ref[...]) + dot_nn(low, uh))


def body(slab, sketch):
    core, row = lax.axis_index(C), lax.axis_index(Y)
    place = jnp.stack([core, row]).astype(jnp.int32)
    tokens, columns = slab.shape[0], sketch.shape[1]
    half, block, strip = tokens // 2, tokens // 8, columns // 4
    halves = slab.reshape(2, half, slab.shape[1])

    def partial(which):
        return jnp.dot(block_of(halves, which), sketch, preferred_element_type=F32)

    theirs = from_partner(partial(1 - core))
    mine = lax.optimization_barrier(partial(core))
    pair_sum = (mine + theirs).reshape(4, block, columns)
    power = jnp.clip(jnp.floor(jnp.log2(jnp.max(jnp.abs(pair_sum)))), -100.0, 40.0)
    own, top = block_of(pair_sum, row), power
    for s in range(1, 4):
        sent = packed(block_of(pair_sum, (row + s) % 4), power)
        values, its_power = unpacked(shifted(sent, Y, s))
        own, top = own + values, jnp.maximum(top, its_power)
    message = packed(own, top + 2.0)
    pieces = [split(unpacked(message)[0])]
    pieces += [split(unpacked(shifted(message, Y, s))[0]) for s in range(1, 4)]

    pair = struct((half, columns), BF16)
    slice_of = struct((strip // 2, columns), F32)
    high_mine, low_mine, kept, given = pl.pallas_call(
        share_kernel,
        out_shape=(pair, pair, slice_of, slice_of),
        in_specs=[SMEM] + [VMEM] * 8,
        out_specs=(VMEM,) * 4,
        scratch_shapes=[pltpu.VMEM((strip, columns), F32)],
        compiler_params=pltpu.CompilerParams(vmem_limit_bytes=16 << 20),
        name="share",
    )(place, *[p[0] for p in pieces], *[p[1] for p in pieces])
    strip_sum = kept + from_partner(given)
    high_other, low_other = from_partner(high_mine), from_partner(low_mine)

    summed = exchange(strip_sum.reshape(8, -1, columns), Z).sum(axis=0)
    summed = (summed + flipped(summed, X, 1)) + (flipped(summed, X, 2) + flipped(summed, X, 3))
    done = exchange(jnp.broadcast_to(summed[None], (8, *summed.shape)), Z).reshape(-1, columns)

    def onto(which, values):
        return dot_tn(block_of(halves, which), values)

    images = onto(core, high_mine) + onto(core, low_mine)
    images = images + (onto(1 - core, high_other) + onto(1 - core, low_other))
    image = exchange(images.astype(BF16).reshape(32, -1, columns), TOK)

    strips = [done] + [shifted(done, Y, s) for s in range(1, 4)]
    square = struct((columns, columns), BF16)
    token_count = tokens * lax.axis_size(TOK)
    q_basis, r_scaled, upper_high, upper_low = pl.pallas_call(
        functools.partial(basis_kernel, 1.0 / math.sqrt(token_count)),
        out_shape=(
            struct((tokens, columns), BF16), struct((columns, columns), F32), square, square
        ),
        in_specs=[SMEM] + [VMEM] * 12,
        out_specs=(VMEM,) * 4,
        scratch_shapes=[pltpu.VMEM((columns, columns), F32)] * 3,
        compiler_params=pltpu.CompilerParams(vmem_limit_bytes=24 << 20),
        name="basis",
    )(place, *strips, *[from_partner(s) for s in strips], high_mine, low_mine, high_other, low_other)
    projected = pl.pallas_call(
        image_kernel,
        out_shape=struct((image.shape[1], columns), F32),
        in_specs=[VMEM] * 3,
        out_specs=VMEM,
        compiler_params=pltpu.CompilerParams(vmem_limit_bytes=8 << 20),
        name="image",
    )(image, upper_high, upper_low)
    return (q_basis, r_scaled, projected)


def solution(mesh):
    split_mesh = Mesh(mesh.devices.reshape(4, 8, 4, 2), (X, Z, Y, C))
    in_specs = (P(TOK, (Y, C)), P((Y, C), None))
    out_specs = (P(TOK, None), P(), P((Y, C, X, Z), None))
    return jax.shard_map(body, mesh=split_mesh, in_specs=in_specs, out_specs=out_specs, check_vma=False)
```

```python
import functools
import math

import jax
import jax.numpy as jnp
from jax import lax
from jax.experimental import pallas as pl
from jax.experimental.pallas import tpu as pltpu
from jax.sharding import Mesh
from jax.sharding import PartitionSpec as P

HIGH = lax.Precision.HIGHEST
NB, PB = 128, 8


def row_of(tile, k):
    return jnp.broadcast_to(tile[k : k + 1, :], (PB, NB))


def diag_factor(block):
    sub = lax.broadcasted_iota(jnp.int32, (PB, NB), 0)
    lane = lax.broadcasted_iota(jnp.int32, (PB, NB), 1)
    n = NB // PB
    xs = [block[PB * p : PB * (p + 1), :] for p in range(n)]
    vs = [jnp.where(lane == sub + PB * p, 1.0, 0.0).astype(jnp.float32) for p in range(n)]
    for p in range(0, n, 2):
        first = PB * p
        x, v = xs[p : p + 2], vs[p : p + 2]
        cols = [
            [jnp.broadcast_to(x[h][:, first + k : first + k + 1], (PB, NB)) for h in range(2)]
            for k in range(2 * PB)
        ]
        scale = [jnp.ones((PB, NB), jnp.float32)] * 2
        for k in range(2 * PB):
            h, i = divmod(k, PB)
            pivot = row_of(cols[k][h], i)
            below = {h: jnp.where(sub > i, cols[k][h], 0.0)}
            if h == 0:
                below[1] = cols[k][1]
            r = lax.rsqrt(pivot)
            square = r * r
            if k + 1 < 2 * PB:
                head = row_of(cols[k + 1][h], i)
                for g in below:
                    cols[k + 1][g] = cols[k + 1][g] - (below[g] * head) * square
            coef = {g: below[g] * square for g in below}
            scale[h] = jnp.where(sub == i, r, scale[h])
            for j in range(k + 2, 2 * PB):
                head = row_of(cols[j][h], i)
                for g in below:
                    cols[j][g] = cols[j][g] - coef[g] * head
            for m in (x, v):
                head = row_of(m[h], i)
                for g in below:
                    m[g] = m[g] - coef[g] * head
        for h in range(2):
            x[h], v[h] = x[h] * scale[h], v[h] * scale[h]
        xs[p : p + 2], vs[p : p + 2] = x, v
        for q in range(p + 2, n):
            pick = lane == sub + PB * q
            for k in range(2 * PB):
                h, i = divmod(k, PB)
                row = row_of(x[h], i)
                c = jnp.sum(jnp.where(pick, row, 0.0), axis=1, keepdims=True)
                xs[q] = xs[q] - c * row
                vs[q] = vs[q] - c * row_of(v[h], i)
    rows = [jnp.where(lane >= sub + PB * p, xs[p], 0.0) for p in range(n)]
    return jnp.concatenate(rows, 0), jnp.concatenate(vs, 0)


def tn(a, b):
    return lax.dot_general(
        a, b, (((0,), (0,)), ((), ())), precision=HIGH, preferred_element_type=jnp.float32
    )


def nn(a, b):
    return jnp.dot(a, b, precision=HIGH, preferred_element_type=jnp.float32)


def factor_in_place(s_ref, r_ref, w_ref):
    n = s_ref.shape[0] // NB

    def at(i):
        return slice(NB * i, NB * (i + 1))

    r_ref[...] = jnp.zeros_like(r_ref)
    w_ref[...] = jnp.zeros_like(w_ref)
    for b in range(n):
        upper, inv = diag_factor(s_ref[at(b), at(b)])
        r_ref[at(b), at(b)] = upper
        w_ref[at(b), at(b)] = inv
        if b < n - 1:
            rest = slice(NB * (b + 1), NB * n)
            r_ref[at(b), rest] = nn(inv, s_ref[at(b), rest])
            for j in range(b + 1, n):
                tail = slice(NB * j, NB * n)
                s_ref[at(j), tail] = s_ref[at(j), tail] - tn(r_ref[at(b), at(j)], r_ref[at(b), tail])
        if b:
            left = tn(r_ref[0 : NB * b, at(b)], w_ref[0 : NB * b, 0 : NB * b])
            w_ref[at(b), 0 : NB * b] = -nn(inv, left)


X, Z, Y, C = "tok_0", "tok_1", "feat_0", "feat_1"
TOK = (X, Z)
LEVEL = 14.0
TAIL = 8
F32, BF16, F16 = jnp.float32, jnp.bfloat16, jnp.float16
VMEM = pl.BlockSpec(memory_space=pltpu.VMEM)
ANY = pl.BlockSpec(memory_space=pl.ANY)
HBM = pl.BlockSpec(memory_space=pltpu.HBM)
SMEM = pl.BlockSpec(memory_space=pltpu.SMEM)


def struct(shape, dtype):
    return jax.ShapeDtypeStruct(shape, dtype)


def exchange(blocks, axis):
    return lax.all_to_all(blocks, axis, 0, 0, tiled=True)


def shifted(array, axis, shift):
    peers = lax.axis_size(axis)
    return lax.ppermute(array, axis, [(i, (i + shift) % peers) for i in range(peers)])


def flipped(array, axis, bit):
    return lax.ppermute(array, axis, [(i, i ^ bit) for i in range(lax.axis_size(axis))])


def from_partner(array):
    return flipped(array, C, 1)


def block_of(blocks, i):
    return lax.dynamic_index_in_dim(blocks, i, 0, keepdims=False)


def tail_of(power, columns):
    i = lax.broadcasted_iota(F32, (TAIL, columns), 0)
    return jnp.exp2(jnp.floor((power - LEVEL + i) / TAIL)).astype(F16)


def unit_of(tail):
    rows = [tail[i : i + 1].astype(F32) for i in range(TAIL)]
    while len(rows) > 1:
        rows = [a * b for a, b in zip(rows[0::2], rows[1::2])]
    return rows[0]


def unpacked(block):
    rows = block.shape[0] - TAIL
    return block[:rows].astype(F32) * unit_of(block[rows:])


def split(values):
    high = lax.reduce_precision(values, 8, 7)
    return high.astype(BF16), (values - high).astype(BF16)


def dot_tn(a, b):
    return lax.dot_general(a, b, (((0,), (0,)), ((), ())), preferred_element_type=F32)


def dot_nn(a, b):
    return jnp.dot(a, b, preferred_element_type=F32)


def part(i, size):
    return pl.ds(pl.multiple_of(i * size, size), size)


def partial_kernel(place_ref, slab_ref, sketch_ref, out_ref):
    out_ref[...] = dot_nn(slab_ref[...], sketch_ref[...])


def share_kernel(place_ref, *refs):
    highs, lows = refs[0:4], refs[4:8]
    high_ref, low_ref, kept_ref, given_ref, strip_ref = refs[8:]
    core, row = place_ref[0], place_ref[1]
    block = highs[0].shape[0]
    for s in range(4):
        at = part(lax.rem(row + 4 - s, 4), block)
        high_ref[at, :] = highs[s][...]
        low_ref[at, :] = lows[s][...]
    strip, half = strip_ref.shape[0], kept_ref.shape[0]
    lanes = part(row, strip)
    high, low = high_ref[...], low_ref[...]
    strip_ref[...] = dot_tn(high_ref[:, lanes], high) + (
        dot_tn(high_ref[:, lanes], low) + dot_tn(low_ref[:, lanes], high)
    )
    kept_ref[...] = strip_ref[part(core, half), :]
    given_ref[...] = strip_ref[part(1 - core, half), :]


def basis_kernel(scale, place_ref, *refs):
    mine, other, sources = refs[0:4], refs[4:8], refs[8:12]
    q_ref, out_ref, uh_ref, ul_ref, s_ref, r_ref, w_ref, y_ref, b_ref, in_sems, out_sems = refs[12:]
    core, row = place_ref[0], place_ref[1]
    half = mine[0].shape[0]
    columns = s_ref.shape[0]
    arriving = [pltpu.make_async_copy(sources[i], y_ref.at[i], in_sems.at[i]) for i in range(4)]
    for copy in arriving:
        copy.start()
    for s in range(4):
        strip = 2 * lax.rem(row + 4 - s, 4)
        s_ref[part(strip + core, half), :] = mine[s][...]
        s_ref[part(strip + 1 - core, half), :] = other[s][...]
    factor_in_place(s_ref, r_ref, w_ref)
    out_ref[...] = r_ref[...] * scale
    for j in range(0, columns, NB):
        u = w_ref[j : j + NB, :].T
        high = u.astype(BF16)
        uh_ref[:, j : j + NB] = high
        ul_ref[:, j : j + NB] = (u - high.astype(F32)).astype(BF16)
    for copy in arriving:
        copy.wait()
    rows, step = y_ref.shape[1], 256
    per = rows // step

    def leaving(i):
        which = lax.div(i, per)
        place = jnp.where(which == 0, core, 1 - core) * per + lax.rem(i, per)
        return pltpu.make_async_copy(b_ref.at[i], q_ref.at[part(place, step)], out_sems.at[i])

    def some_rows(i, _):
        which, at = lax.div(i, per), part(lax.rem(i, per), step)
        for j in range(0, columns, 256):
            k = j + 256
            h, l = y_ref[2 * which, at, :k], y_ref[2 * which + 1, at, :k]
            uh, ul = uh_ref[:k, j:k], ul_ref[:k, j:k]
            b_ref[i, :, j:k] = (dot_nn(h, uh) + (dot_nn(h, ul) + dot_nn(l, uh))).astype(BF16)
        leaving(i).start()
        return 0

    lax.fori_loop(0, 2 * per, some_rows, 0)
    for i in range(2 * per):
        leaving(i).wait()


def project_kernel(place_ref, slab_ref, hm_ref, lm_ref, ho_ref, lo_ref, out_ref):
    core, rows = place_ref[0], hm_ref.shape[0]
    a, b = slab_ref[part(core, rows), :], slab_ref[part(1 - core, rows), :]
    total = (dot_tn(a, hm_ref[...]) + dot_tn(b, ho_ref[...])) + (
        dot_tn(a, lm_ref[...]) + dot_tn(b, lo_ref[...])
    )
    out_ref[...] = total.astype(BF16)


def image_kernel(in_any, uh_any, ul_any, out_ref, in_ref, uh_ref, ul_ref, sems):
    pairs = ((in_any, in_ref), (uh_any, uh_ref), (ul_any, ul_ref))
    copies = [pltpu.make_async_copy(a, b, sems.at[i]) for i, (a, b) in enumerate(pairs)]
    for copy in copies:
        copy.start()
    for copy in copies:
        copy.wait()
    total = in_ref[0].astype(F32)
    for i in range(1, in_ref.shape[0]):
        total = total + in_ref[i].astype(F32)
    high = total.astype(BF16)
    low = (total - high.astype(F32)).astype(BF16)
    uh = uh_ref[...]
    out_ref[...] = dot_nn(high, uh) + (dot_nn(high, ul_ref[...]) + dot_nn(low, uh))


def body(slab, sketch):
    core, row = lax.axis_index(C), lax.axis_index(Y)
    place = jnp.stack([core, row]).astype(jnp.int32)
    tokens, columns = slab.shape[0], sketch.shape[1]
    half, block, strip = tokens // 2, tokens // 8, columns // 4

    def partial(which):
        tile = 256
        first = lambda i, place: (place[0] * (half // tile) + i, 0)
        return pl.pallas_call(
            partial_kernel,
            out_shape=struct((half, columns), F32),
            grid_spec=pltpu.PrefetchScalarGridSpec(
                num_scalar_prefetch=1,
                grid=(half // tile,),
                in_specs=[
                    pl.BlockSpec((tile, slab.shape[1]), first),
                    pl.BlockSpec(sketch.shape, lambda i, place: (0, 0)),
                ],
                out_specs=pl.BlockSpec((tile, columns), lambda i, place: (i, 0)),
            ),
            compiler_params=pltpu.CompilerParams(vmem_limit_bytes=16 << 20),
            cost_estimate=pl.CostEstimate(
                flops=2 * half * slab.shape[1] * columns,
                bytes_accessed=2 * half * slab.shape[1] + 4 * half * columns,
                transcendentals=0,
            ),
            name="partial",
        )(jnp.reshape(which, (1,)).astype(jnp.int32), slab, sketch)

    theirs = from_partner(partial(1 - core))
    pair_sum = (partial(core) + theirs).reshape(4, block, columns)
    power = jnp.clip(jnp.floor(jnp.log2(jnp.max(jnp.abs(pair_sum)))), 16.0 - 8 * LEVEL, 40.0)
    lift = jnp.exp2(LEVEL - power)
    tail = tail_of(power, columns)
    own, top = block_of(pair_sum, row), tail
    for s in range(1, 4):
        values = (block_of(pair_sum, (row + s) % 4) * lift).astype(F16)
        got = shifted(jnp.concatenate([values, tail]), Y, s)
        own, top = own + unpacked(got), jnp.maximum(top, got[block:])
    top = jnp.where(lax.broadcasted_iota(jnp.int32, top.shape, 0) < 2, top * 2, top)
    message = jnp.concatenate([(own / unit_of(top)).astype(F16), top])
    pieces = [split(unpacked(message))]
    pieces += [split(unpacked(shifted(message, Y, s))) for s in range(1, 4)]

    pair = struct((half, columns), BF16)
    slice_of = struct((strip // 2, columns), F32)
    high_mine, low_mine, kept, given = pl.pallas_call(
        share_kernel,
        out_shape=(pair, pair, slice_of, slice_of),
        in_specs=[SMEM] + [VMEM] * 8,
        out_specs=(VMEM,) * 4,
        scratch_shapes=[pltpu.VMEM((strip, columns), F32)],
        compiler_params=pltpu.CompilerParams(vmem_limit_bytes=16 << 20),
        name="share",
    )(place, *[p[0] for p in pieces], *[p[1] for p in pieces])
    strip_sum = kept + from_partner(given)
    high_other, low_other = from_partner(high_mine), from_partner(low_mine)

    features = slab.shape[1]
    tile = 256
    whole = pl.BlockSpec((half, columns), lambda i: (0, 0))
    images = pl.pallas_call(
        project_kernel,
        out_shape=struct((features, columns), BF16),
        grid=(features // tile,),
        in_specs=[SMEM, pl.BlockSpec((tokens, tile), lambda i: (0, i))] + [whole] * 4,
        out_specs=pl.BlockSpec((tile, columns), lambda i: (i, 0)),
        compiler_params=pltpu.CompilerParams(vmem_limit_bytes=24 << 20),
        cost_estimate=pl.CostEstimate(
            flops=4 * tokens * features * columns,
            bytes_accessed=2 * tokens * (features + 2 * columns) + 2 * features * columns,
            transcendentals=0,
        ),
        name="project",
    )(place, slab, high_mine, low_mine, high_other, low_other)

    arrived = exchange(strip_sum.reshape(8, -1, columns), Z)
    arrived, images = lax.optimization_barrier((arrived, images))
    summed = arrived.sum(axis=0)
    summed = (summed + flipped(summed, X, 1)) + (flipped(summed, X, 2) + flipped(summed, X, 3))
    done = exchange(jnp.broadcast_to(summed[None], (8, *summed.shape)), Z).reshape(-1, columns)

    strips = [done]
    for s in range(1, 4):
        strips.append(shifted(done, Y, s))
    others = [from_partner(s) for s in strips]
    image = exchange(images.reshape(32, -1, columns), TOK)

    square = struct((columns, columns), BF16)
    token_count = tokens * lax.axis_size(TOK)
    q_basis, r_scaled, upper_high, upper_low = pl.pallas_call(
        functools.partial(basis_kernel, 1.0 / math.sqrt(token_count)),
        out_shape=(
            struct((tokens, columns), BF16), struct((columns, columns), F32), square, square
        ),
        in_specs=[SMEM] + [VMEM] * 8 + [HBM] * 4,
        out_specs=(ANY,) + (VMEM,) * 3,
        scratch_shapes=[pltpu.VMEM((columns, columns), F32)] * 3
        + [
            pltpu.VMEM((4, half, columns), BF16),
            pltpu.VMEM((8, tokens // 8, columns), BF16),
            pltpu.SemaphoreType.DMA((4,)),
            pltpu.SemaphoreType.DMA((8,)),
        ],
        compiler_params=pltpu.CompilerParams(vmem_limit_bytes=24 << 20),
        cost_estimate=pl.CostEstimate(
            flops=20 * tokens * columns * columns,
            bytes_accessed=16 * tokens * columns,
            transcendentals=0,
        ),
        name="basis",
    )(place, *strips, *others, high_mine, low_mine, high_other, low_other)
    projected = pl.pallas_call(
        image_kernel,
        out_shape=struct((image.shape[1], columns), F32),
        in_specs=[ANY] * 3,
        out_specs=VMEM,
        scratch_shapes=[
            pltpu.VMEM(image.shape, BF16),
            pltpu.VMEM((columns, columns), BF16),
            pltpu.VMEM((columns, columns), BF16),
            pltpu.SemaphoreType.DMA((3,)),
        ],
        compiler_params=pltpu.CompilerParams(vmem_limit_bytes=12 << 20),
        name="image",
    )(image, upper_high, upper_low)
    return (q_basis, r_scaled, projected)


def solution(mesh):
    split_mesh = Mesh(mesh.devices.reshape(4, 8, 4, 2), (X, Z, Y, C))
    in_specs = (P(TOK, (Y, C)), P((Y, C), None))
    out_specs = (P(TOK, None), P(), P((Y, C, X, Z), None))
    return jax.shard_map(body, mesh=split_mesh, in_specs=in_specs, out_specs=out_specs, check_vma=False)
```

```python
import functools
import math

import jax
import jax.numpy as jnp
from jax import lax
from jax.experimental import pallas as pl
from jax.experimental.pallas import tpu as pltpu
from jax.sharding import Mesh
from jax.sharding import PartitionSpec as P

HIGH = lax.Precision.HIGHEST
NB, PB = 128, 8


def row_of(tile, k):
    return jnp.broadcast_to(tile[k : k + 1, :], (PB, NB))


def diag_factor(block):
    sub = lax.broadcasted_iota(jnp.int32, (PB, NB), 0)
    lane = lax.broadcasted_iota(jnp.int32, (PB, NB), 1)
    n = NB // PB
    xs = [block[PB * p : PB * (p + 1), :] for p in range(n)]
    vs = [jnp.where(lane == sub + PB * p, 1.0, 0.0).astype(jnp.float32) for p in range(n)]
    for p in range(0, n, 2):
        first = PB * p
        x, v = xs[p : p + 2], vs[p : p + 2]
        cols = [
            [jnp.broadcast_to(x[h][:, first + k : first + k + 1], (PB, NB)) for h in range(2)]
            for k in range(2 * PB)
        ]
        scale = [jnp.ones((PB, NB), jnp.float32)] * 2
        for k in range(2 * PB):
            h, i = divmod(k, PB)
            pivot = row_of(cols[k][h], i)
            below = {h: jnp.where(sub > i, cols[k][h], 0.0)}
            if h == 0:
                below[1] = cols[k][1]
            r = lax.rsqrt(pivot)
            square = r * r
            if k + 1 < 2 * PB:
                head = row_of(cols[k + 1][h], i)
                for g in below:
                    cols[k + 1][g] = cols[k + 1][g] - (below[g] * head) * square
            coef = {g: below[g] * square for g in below}
            scale[h] = jnp.where(sub == i, r, scale[h])
            for j in range(k + 2, 2 * PB):
                head = row_of(cols[j][h], i)
                for g in below:
                    cols[j][g] = cols[j][g] - coef[g] * head
            for m in (x, v):
                head = row_of(m[h], i)
                for g in below:
                    m[g] = m[g] - coef[g] * head
        for h in range(2):
            x[h], v[h] = x[h] * scale[h], v[h] * scale[h]
        xs[p : p + 2], vs[p : p + 2] = x, v
        for q in range(p + 2, n):
            pick = lane == sub + PB * q
            for k in range(2 * PB):
                h, i = divmod(k, PB)
                row = row_of(x[h], i)
                c = jnp.sum(jnp.where(pick, row, 0.0), axis=1, keepdims=True)
                xs[q] = xs[q] - c * row
                vs[q] = vs[q] - c * row_of(v[h], i)
    rows = [jnp.where(lane >= sub + PB * p, xs[p], 0.0) for p in range(n)]
    return jnp.concatenate(rows, 0), jnp.concatenate(vs, 0)


def tn(a, b):
    return lax.dot_general(
        a, b, (((0,), (0,)), ((), ())), precision=HIGH, preferred_element_type=jnp.float32
    )


def nn(a, b):
    return jnp.dot(a, b, precision=HIGH, preferred_element_type=jnp.float32)


def factor_in_place(s_ref, r_ref, w_ref):
    n = s_ref.shape[0] // NB

    def at(i):
        return slice(NB * i, NB * (i + 1))

    r_ref[...] = jnp.zeros_like(r_ref)
    w_ref[...] = jnp.zeros_like(w_ref)
    for b in range(n):
        upper, inv = diag_factor(s_ref[at(b), at(b)])
        r_ref[at(b), at(b)] = upper
        w_ref[at(b), at(b)] = inv
        if b < n - 1:
            rest = slice(NB * (b + 1), NB * n)
            r_ref[at(b), rest] = nn(inv, s_ref[at(b), rest])
            for j in range(b + 1, n):
                tail = slice(NB * j, NB * n)
                s_ref[at(j), tail] = s_ref[at(j), tail] - tn(r_ref[at(b), at(j)], r_ref[at(b), tail])
        if b:
            left = tn(r_ref[0 : NB * b, at(b)], w_ref[0 : NB * b, 0 : NB * b])
            w_ref[at(b), 0 : NB * b] = -nn(inv, left)


X, Z, Y, C = "tok_0", "tok_1", "feat_0", "feat_1"
TOK = (X, Z)
LEVEL = 14.0
TAIL = 8
ROOMY = 56 << 20
F32, BF16, F16 = jnp.float32, jnp.bfloat16, jnp.float16
VMEM = pl.BlockSpec(memory_space=pltpu.VMEM)
ANY = pl.BlockSpec(memory_space=pl.ANY)
HBM = pl.BlockSpec(memory_space=pltpu.HBM)
SMEM = pl.BlockSpec(memory_space=pltpu.SMEM)


def struct(shape, dtype):
    return jax.ShapeDtypeStruct(shape, dtype)


def exchange(blocks, axis):
    return lax.all_to_all(blocks, axis, 0, 0, tiled=True)


def shifted(array, axis, shift):
    peers = lax.axis_size(axis)
    return lax.ppermute(array, axis, [(i, (i + shift) % peers) for i in range(peers)])


def flipped(array, axis, bit):
    return lax.ppermute(array, axis, [(i, i ^ bit) for i in range(lax.axis_size(axis))])


def from_partner(array):
    return flipped(array, C, 1)


def block_of(blocks, i):
    return lax.dynamic_index_in_dim(blocks, i, 0, keepdims=False)


def tail_of(power, columns):
    i = lax.broadcasted_iota(F32, (TAIL, columns), 0)
    return jnp.exp2(jnp.floor((power - LEVEL + i) / TAIL)).astype(F16)


def unit_of(tail):
    rows = [tail[i : i + 1].astype(F32) for i in range(TAIL)]
    while len(rows) > 1:
        rows = [a * b for a, b in zip(rows[0::2], rows[1::2])]
    return rows[0]


def unpacked(block):
    rows = block.shape[0] - TAIL
    return block[:rows].astype(F32) * unit_of(block[rows:])


def split(values):
    high = lax.reduce_precision(values, 8, 7)
    return high.astype(BF16), (values - high).astype(BF16)


def dot_tn(a, b):
    return lax.dot_general(a, b, (((0,), (0,)), ((), ())), preferred_element_type=F32)


def dot_nn(a, b):
    return jnp.dot(a, b, preferred_element_type=F32)


def part(i, size):
    return pl.ds(pl.multiple_of(i * size, size), size)


def partial_kernel(place_ref, slab_ref, sketch_ref, out_ref, top_ref):
    product = dot_nn(slab_ref[...], sketch_ref[...])
    out_ref[...] = product
    top = jnp.max(jnp.max(jnp.abs(product), axis=0, keepdims=True), axis=1, keepdims=True)
    top_ref[...] = jnp.broadcast_to(top, top_ref.shape)


def share_kernel(place_ref, *refs):
    highs, lows = refs[0:4], refs[4:8]
    high_ref, low_ref, kept_ref, given_ref, strip_ref = refs[8:]
    core, row = place_ref[0], place_ref[1]
    block = highs[0].shape[0]
    for s in range(4):
        at = part(lax.rem(row + 4 - s, 4), block)
        high_ref[at, :] = highs[s][...]
        low_ref[at, :] = lows[s][...]
    strip, half = strip_ref.shape[0], kept_ref.shape[0]
    lanes = part(row, strip)
    high, low = high_ref[...], low_ref[...]
    strip_ref[...] = dot_tn(high_ref[:, lanes], high) + (
        dot_tn(high_ref[:, lanes], low) + dot_tn(low_ref[:, lanes], high)
    )
    kept_ref[...] = strip_ref[part(core, half), :]
    given_ref[...] = strip_ref[part(1 - core, half), :]


def basis_kernel(scale, place_ref, *refs):
    mine, other, sources = refs[0:4], refs[4:8], refs[8:12]
    q_ref, r_any, uh_any, ul_any = refs[12:16]
    s_ref, r_ref, w_ref, uh_ref, ul_ref, y_ref, b_ref, strip_sems, in_sems, small_sems, out_sems = refs[16:]
    core, row = place_ref[0], place_ref[1]
    half = mine[0].shape[0]
    columns = s_ref.shape[0]
    strips = []
    for s in range(4):
        strip = 2 * lax.rem(row + 4 - s, 4)
        for ref, side in ((mine[s], core), (other[s], 1 - core)):
            there = s_ref.at[part(strip + side, half)]
            strips.append(pltpu.make_async_copy(ref, there, strip_sems.at[len(strips)]))
    arriving = [pltpu.make_async_copy(sources[i], y_ref.at[i], in_sems.at[i]) for i in range(4)]
    for copy in strips + arriving:
        copy.start()
    for copy in strips:
        copy.wait()
    factor_in_place(s_ref, r_ref, w_ref)
    r_ref[...] = r_ref[...] * scale
    for j in range(0, columns, NB):
        u = w_ref[j : j + NB, :].T
        high = u.astype(BF16)
        uh_ref[:, j : j + NB] = high
        ul_ref[:, j : j + NB] = (u - high.astype(F32)).astype(BF16)
    pairs = ((r_ref, r_any), (uh_ref, uh_any), (ul_ref, ul_any))
    small = [pltpu.make_async_copy(a, b, small_sems.at[i]) for i, (a, b) in enumerate(pairs)]
    for copy in small:
        copy.start()
    for copy in arriving:
        copy.wait()
    rows, step = y_ref.shape[1], 256
    per = rows // step

    def leaving(i):
        which = lax.div(i, per)
        place = jnp.where(which == 0, core, 1 - core) * per + lax.rem(i, per)
        return pltpu.make_async_copy(b_ref.at[i], q_ref.at[part(place, step)], out_sems.at[i])

    def some_rows(i, _):
        which, at = lax.div(i, per), part(lax.rem(i, per), step)
        for j in range(0, columns, 256):
            k = j + 256
            h, l = y_ref[2 * which, at, :k], y_ref[2 * which + 1, at, :k]
            uh, ul = uh_ref[:k, j:k], ul_ref[:k, j:k]
            b_ref[i, :, j:k] = (dot_nn(h, uh) + (dot_nn(h, ul) + dot_nn(l, uh))).astype(BF16)
        leaving(i).start()
        return 0

    lax.fori_loop(0, 2 * per, some_rows, 0)
    for i in range(2 * per):
        leaving(i).wait()
    for copy in small:
        copy.wait()


def project_kernel(place_ref, slab_ref, hm_ref, lm_ref, ho_ref, lo_ref, *refs):
    out_ref = refs[-1]
    core, rows = place_ref[0], hm_ref.shape[0]
    a, b = slab_ref[part(core, rows), :], slab_ref[part(1 - core, rows), :]
    total = (dot_tn(a, hm_ref[...]) + dot_tn(b, ho_ref[...])) + (
        dot_tn(a, lm_ref[...]) + dot_tn(b, lo_ref[...])
    )
    out_ref[...] = total.astype(BF16)


def image_kernel(in_any, uh_any, ul_any, out_ref, in_ref, uh_ref, ul_ref, sems):
    pairs = ((in_any, in_ref), (uh_any, uh_ref), (ul_any, ul_ref))
    copies = [pltpu.make_async_copy(a, b, sems.at[i]) for i, (a, b) in enumerate(pairs)]
    for copy in copies:
        copy.start()
    for copy in copies:
        copy.wait()
    total = in_ref[0].astype(F32)
    for i in range(1, in_ref.shape[0]):
        total = total + in_ref[i].astype(F32)
    high = total.astype(BF16)
    low = (total - high.astype(F32)).astype(BF16)
    uh = uh_ref[...]
    out_ref[...] = dot_nn(high, uh) + (dot_nn(high, ul_ref[...]) + dot_nn(low, uh))


def body(slab, sketch):
    core, row = lax.axis_index(C), lax.axis_index(Y)
    place = jnp.stack([core, row]).astype(jnp.int32)
    tokens, columns = slab.shape[0], sketch.shape[1]
    half, block, strip = tokens // 2, tokens // 8, columns // 4

    def partial(which):
        tile = 256
        first = lambda i, place: (place[0] * (half // tile) + i, 0)
        steps = half // tile
        return pl.pallas_call(
            partial_kernel,
            out_shape=(struct((half, columns), F32), struct((8 * steps, 128), F32)),
            grid_spec=pltpu.PrefetchScalarGridSpec(
                num_scalar_prefetch=1,
                grid=(steps,),
                in_specs=[
                    pl.BlockSpec((tile, slab.shape[1]), first),
                    pl.BlockSpec(sketch.shape, lambda i, place: (0, 0)),
                ],
                out_specs=(
                    pl.BlockSpec((tile, columns), lambda i, place: (i, 0)),
                    pl.BlockSpec((8, 128), lambda i, place: (i, 0)),
                ),
            ),
            compiler_params=pltpu.CompilerParams(vmem_limit_bytes=ROOMY),
            cost_estimate=pl.CostEstimate(
                flops=2 * half * slab.shape[1] * columns,
                bytes_accessed=2 * half * slab.shape[1] + 4 * half * columns,
                transcendentals=0,
            ),
            name="partial",
        )(jnp.reshape(which, (1,)).astype(jnp.int32), slab, sketch)

    given, given_top = partial(1 - core)
    theirs, theirs_top = from_partner(given), from_partner(given_top)
    mine, mine_top = partial(core)
    mine, theirs = mine.reshape(4, block, columns), theirs.reshape(4, block, columns)
    top = jnp.max(mine_top) + jnp.max(theirs_top)
    power = jnp.clip(jnp.floor(jnp.log2(top)), 16.0 - 8 * LEVEL, 40.0)
    lift = jnp.exp2(LEVEL - power)
    tail = tail_of(power, columns)

    def pair_sum(i):
        return block_of(mine, i) + block_of(theirs, i)

    own, top = pair_sum(row), tail
    for s in range(1, 4):
        values = (pair_sum((row + s) % 4) * lift).astype(F16)
        got = shifted(jnp.concatenate([values, tail]), Y, s)
        own, top = own + unpacked(got), jnp.maximum(top, got[block:])
    top = jnp.where(lax.broadcasted_iota(jnp.int32, top.shape, 0) < 2, top * 2, top)
    message = jnp.concatenate([(own / unit_of(top)).astype(F16), top])
    pieces = [split(unpacked(message))]
    pieces += [split(unpacked(shifted(message, Y, s))) for s in range(1, 4)]

    pair = struct((half, columns), BF16)
    slice_of = struct((strip // 2, columns), F32)
    high_mine, low_mine, kept, given = pl.pallas_call(
        share_kernel,
        out_shape=(pair, pair, slice_of, slice_of),
        in_specs=[SMEM] + [VMEM] * 8,
        out_specs=(VMEM,) * 4,
        scratch_shapes=[pltpu.VMEM((strip, columns), F32)],
        compiler_params=pltpu.CompilerParams(vmem_limit_bytes=16 << 20),
        name="share",
    )(place, *[p[0] for p in pieces], *[p[1] for p in pieces])
    strip_sum = kept + from_partner(given)
    high_mine, low_mine, strip_sum = lax.optimization_barrier((high_mine, low_mine, strip_sum))
    high_other, low_other = from_partner(high_mine), from_partner(low_mine)

    features = slab.shape[1]
    tile = 256

    def project(first, images):
        steps = features // tile // 2
        whole = pl.BlockSpec((half, columns), lambda i: (0, 0))
        return pl.pallas_call(
            project_kernel,
            out_shape=struct((features, columns), BF16),
            grid=(steps,),
            in_specs=[SMEM, pl.BlockSpec((tokens, tile), lambda i: (0, first * steps + i))]
            + [whole] * 4
            + [ANY] * len(images),
            out_specs=pl.BlockSpec((tile, columns), lambda i: (first * steps + i, 0)),
            input_output_aliases={6: 0} if images else {},
            compiler_params=pltpu.CompilerParams(vmem_limit_bytes=ROOMY),
            cost_estimate=pl.CostEstimate(
                flops=2 * tokens * features * columns,
                bytes_accessed=tokens * (features + 4 * columns) + features * columns,
                transcendentals=0,
            ),
        )(place, slab, high_mine, low_mine, high_other, low_other, *images)

    arrived = exchange(strip_sum.reshape(8, -1, columns), Z)
    images = project(0, ())
    arrived, images = lax.optimization_barrier((arrived, images))
    summed = arrived.sum(axis=0)
    summed = (summed + flipped(summed, X, 1)) + (flipped(summed, X, 2) + flipped(summed, X, 3))
    done = exchange(jnp.broadcast_to(summed[None], (8, *summed.shape)), Z)
    images = project(1, (images,))
    done, images = lax.optimization_barrier((done, images))
    done = done.reshape(-1, columns)

    strips = [done]
    for s in range(1, 4):
        strips.append(shifted(done, Y, s))
    others = [from_partner(s) for s in strips]
    image = exchange(images.reshape(32, -1, columns), TOK)

    square = struct((columns, columns), BF16)
    token_count = tokens * lax.axis_size(TOK)
    q_basis, r_scaled, upper_high, upper_low = pl.pallas_call(
        functools.partial(basis_kernel, 1.0 / math.sqrt(token_count)),
        out_shape=(
            struct((tokens, columns), BF16), struct((columns, columns), F32), square, square
        ),
        in_specs=[SMEM] + [ANY] * 12,
        out_specs=(ANY,) * 4,
        scratch_shapes=[pltpu.VMEM((columns, columns), F32)] * 3
        + [pltpu.VMEM((columns, columns), BF16)] * 2
        + [
            pltpu.VMEM((4, half, columns), BF16),
            pltpu.VMEM((8, tokens // 8, columns), BF16),
            pltpu.SemaphoreType.DMA((8,)),
            pltpu.SemaphoreType.DMA((4,)),
            pltpu.SemaphoreType.DMA((3,)),
            pltpu.SemaphoreType.DMA((8,)),
        ],
        compiler_params=pltpu.CompilerParams(vmem_limit_bytes=ROOMY),
        cost_estimate=pl.CostEstimate(
            flops=20 * tokens * columns * columns,
            bytes_accessed=16 * tokens * columns,
            transcendentals=0,
        ),
        name="basis",
    )(place, *strips, *others, high_mine, low_mine, high_other, low_other)
    projected = pl.pallas_call(
        image_kernel,
        out_shape=struct((image.shape[1], columns), F32),
        in_specs=[ANY] * 3,
        out_specs=VMEM,
        scratch_shapes=[
            pltpu.VMEM(image.shape, BF16),
            pltpu.VMEM((columns, columns), BF16),
            pltpu.VMEM((columns, columns), BF16),
            pltpu.SemaphoreType.DMA((3,)),
        ],
        compiler_params=pltpu.CompilerParams(vmem_limit_bytes=ROOMY),
        name="image",
    )(image, upper_high, upper_low)
    return (q_basis, r_scaled, projected)


def solution(mesh):
    split_mesh = Mesh(mesh.devices.reshape(4, 8, 4, 2), (X, Z, Y, C))
    in_specs = (P(TOK, (Y, C)), P((Y, C), None))
    out_specs = (P(TOK, None), P(), P((Y, C, X, Z), None))
    return jax.shard_map(body, mesh=split_mesh, in_specs=in_specs, out_specs=out_specs, check_vma=False)
```

```python
import functools
import math

import jax
import jax.numpy as jnp
from jax import lax
from jax.experimental import pallas as pl
from jax.experimental.pallas import tpu as pltpu
from jax.sharding import Mesh
from jax.sharding import PartitionSpec as P

HIGH = lax.Precision.HIGHEST
NB, PB = 128, 8


def row_of(tile, k):
    return jnp.broadcast_to(tile[k : k + 1, :], (PB, NB))


def diag_factor(block):
    sub = lax.broadcasted_iota(jnp.int32, (PB, NB), 0)
    lane = lax.broadcasted_iota(jnp.int32, (PB, NB), 1)
    n = NB // PB
    xs = [block[PB * p : PB * (p + 1), :] for p in range(n)]
    vs = [jnp.where(lane == sub + PB * p, 1.0, 0.0).astype(jnp.float32) for p in range(n)]
    for p in range(0, n, 2):
        first = PB * p
        x, v = xs[p : p + 2], vs[p : p + 2]
        cols = [
            [jnp.broadcast_to(x[h][:, first + k : first + k + 1], (PB, NB)) for h in range(2)]
            for k in range(2 * PB)
        ]
        scale = [jnp.ones((PB, NB), jnp.float32)] * 2
        for k in range(2 * PB):
            h, i = divmod(k, PB)
            pivot = row_of(cols[k][h], i)
            below = {h: jnp.where(sub > i, cols[k][h], 0.0)}
            if h == 0:
                below[1] = cols[k][1]
            r = lax.rsqrt(pivot)
            square = r * r
            if k + 1 < 2 * PB:
                head = row_of(cols[k + 1][h], i)
                for g in below:
                    cols[k + 1][g] = cols[k + 1][g] - (below[g] * head) * square
            coef = {g: below[g] * square for g in below}
            scale[h] = jnp.where(sub == i, r, scale[h])
            for j in range(k + 2, 2 * PB):
                head = row_of(cols[j][h], i)
                for g in below:
                    cols[j][g] = cols[j][g] - coef[g] * head
            for m in (x, v):
                head = row_of(m[h], i)
                for g in below:
                    m[g] = m[g] - coef[g] * head
        for h in range(2):
            x[h], v[h] = x[h] * scale[h], v[h] * scale[h]
        xs[p : p + 2], vs[p : p + 2] = x, v
        for q in range(p + 2, n):
            pick = lane == sub + PB * q
            for k in range(2 * PB):
                h, i = divmod(k, PB)
                row = row_of(x[h], i)
                c = jnp.sum(jnp.where(pick, row, 0.0), axis=1, keepdims=True)
                xs[q] = xs[q] - c * row
                vs[q] = vs[q] - c * row_of(v[h], i)
    rows = [jnp.where(lane >= sub + PB * p, xs[p], 0.0) for p in range(n)]
    return jnp.concatenate(rows, 0), jnp.concatenate(vs, 0)


def tn(a, b):
    return lax.dot_general(
        a, b, (((0,), (0,)), ((), ())), precision=HIGH, preferred_element_type=jnp.float32
    )


def nn(a, b):
    return jnp.dot(a, b, precision=HIGH, preferred_element_type=jnp.float32)


def factor_in_place(s_ref, r_ref, w_ref):
    n = s_ref.shape[0] // NB

    def at(i):
        return slice(NB * i, NB * (i + 1))

    r_ref[...] = jnp.zeros_like(r_ref)
    w_ref[...] = jnp.zeros_like(w_ref)
    for b in range(n):
        upper, inv = diag_factor(s_ref[at(b), at(b)])
        r_ref[at(b), at(b)] = upper
        w_ref[at(b), at(b)] = inv
        if b < n - 1:
            rest = slice(NB * (b + 1), NB * n)
            r_ref[at(b), rest] = nn(inv, s_ref[at(b), rest])
            for j in range(b + 1, n):
                tail = slice(NB * j, NB * n)
                s_ref[at(j), tail] = s_ref[at(j), tail] - tn(r_ref[at(b), at(j)], r_ref[at(b), tail])
        if b:
            left = tn(r_ref[0 : NB * b, at(b)], w_ref[0 : NB * b, 0 : NB * b])
            w_ref[at(b), 0 : NB * b] = -nn(inv, left)


X, Z, Y, C = "tok_0", "tok_1", "feat_0", "feat_1"
TOK = (X, Z)
LEVEL = 14.0
TAIL = 8
ROOMY = 56 << 20
F32, BF16, F16 = jnp.float32, jnp.bfloat16, jnp.float16
VMEM = pl.BlockSpec(memory_space=pltpu.VMEM)
ANY = pl.BlockSpec(memory_space=pl.ANY)
HBM = pl.BlockSpec(memory_space=pltpu.HBM)
SMEM = pl.BlockSpec(memory_space=pltpu.SMEM)


def struct(shape, dtype):
    return jax.ShapeDtypeStruct(shape, dtype)


def exchange(blocks, axis):
    return lax.all_to_all(blocks, axis, 0, 0, tiled=True)


def shifted(array, axis, shift):
    peers = lax.axis_size(axis)
    return lax.ppermute(array, axis, [(i, (i + shift) % peers) for i in range(peers)])


def flipped(array, axis, bit):
    return lax.ppermute(array, axis, [(i, i ^ bit) for i in range(lax.axis_size(axis))])


def from_partner(array):
    return flipped(array, C, 1)


def block_of(blocks, i):
    return lax.dynamic_index_in_dim(blocks, i, 0, keepdims=False)


def tail_of(power, columns):
    i = lax.broadcasted_iota(F32, (TAIL, columns), 0)
    return jnp.exp2(jnp.floor((power - LEVEL + i) / TAIL)).astype(F16)


def unit_of(tail):
    rows = [tail[i : i + 1].astype(F32) for i in range(TAIL)]
    while len(rows) > 1:
        rows = [a * b for a, b in zip(rows[0::2], rows[1::2])]
    return rows[0]


def unpacked(block):
    rows = block.shape[0] - TAIL
    return block[:rows].astype(F32) * unit_of(block[rows:])


def split(values):
    high = lax.reduce_precision(values, 8, 7)
    return high.astype(BF16), (values - high).astype(BF16)


def dot_tn(a, b):
    return lax.dot_general(a, b, (((0,), (0,)), ((), ())), preferred_element_type=F32)


def dot_nn(a, b):
    return jnp.dot(a, b, preferred_element_type=F32)


def part(i, size):
    return pl.ds(pl.multiple_of(i * size, size), size)


def partial_kernel(place_ref, slab_ref, sketch_ref, out_ref):
    out_ref[...] = dot_nn(slab_ref[...], sketch_ref[...])


def share_kernel(place_ref, *refs):
    highs, lows = refs[0:4], refs[4:8]
    high_ref, low_ref, kept_ref, given_ref, strip_ref = refs[8:]
    core, row = place_ref[0], place_ref[1]
    block = highs[0].shape[0]
    for s in range(4):
        at = part(lax.rem(row + 4 - s, 4), block)
        high_ref[at, :] = highs[s][...]
        low_ref[at, :] = lows[s][...]
    strip, half = strip_ref.shape[0], kept_ref.shape[0]
    lanes = part(row, strip)
    high, low = high_ref[...], low_ref[...]
    strip_ref[...] = dot_tn(high_ref[:, lanes], high) + (
        dot_tn(high_ref[:, lanes], low) + dot_tn(low_ref[:, lanes], high)
    )
    kept_ref[...] = strip_ref[part(core, half), :]
    given_ref[...] = strip_ref[part(1 - core, half), :]


def basis_kernel(scale, place_ref, *refs):
    mine, other, sources = refs[0:4], refs[4:8], refs[8:12]
    q_ref, r_any, u_ref = refs[12:15]
    uh_ref, ul_ref = u_ref.at[0], u_ref.at[1]
    s_ref, r_ref, w_ref, y_ref, b_ref, strip_sems, in_sems, scaled_sem, out_sems = refs[15:]
    core, row = place_ref[0], place_ref[1]
    half = mine[0].shape[0]
    columns = s_ref.shape[0]
    strips = []
    for s in range(4):
        strip = 2 * lax.rem(row + 4 - s, 4)
        for ref, side in ((mine[s], core), (other[s], 1 - core)):
            there = s_ref.at[part(strip + side, half)]
            strips.append(pltpu.make_async_copy(ref, there, strip_sems.at[len(strips)]))
    arriving = [pltpu.make_async_copy(sources[i], y_ref.at[i], in_sems.at[i]) for i in range(4)]
    for copy in strips + arriving:
        copy.start()
    for copy in strips:
        copy.wait()
    factor_in_place(s_ref, r_ref, w_ref)
    r_ref[...] = r_ref[...] * scale
    for j in range(0, columns, NB):
        u = w_ref[j : j + NB, :].T
        high = u.astype(BF16)
        uh_ref[:, j : j + NB] = high
        ul_ref[:, j : j + NB] = (u - high.astype(F32)).astype(BF16)
    scaled = pltpu.make_async_copy(r_ref, r_any, scaled_sem)
    scaled.start()
    for copy in arriving:
        copy.wait()
    rows, step = y_ref.shape[1], 256
    per = rows // step

    def leaving(i):
        which = lax.div(i, per)
        place = jnp.where(which == 0, core, 1 - core) * per + lax.rem(i, per)
        return pltpu.make_async_copy(b_ref.at[i], q_ref.at[part(place, step)], out_sems.at[i])

    def some_rows(i, _):
        which, at = lax.div(i, per), part(lax.rem(i, per), step)
        for j in range(0, columns, 256):
            k = j + 256
            h, l = y_ref[2 * which, at, :k], y_ref[2 * which + 1, at, :k]
            uh, ul = uh_ref[:k, j:k], ul_ref[:k, j:k]
            b_ref[i, :, j:k] = (dot_nn(h, uh) + (dot_nn(h, ul) + dot_nn(l, uh))).astype(BF16)
        leaving(i).start()
        return 0

    lax.fori_loop(0, 2 * per, some_rows, 0)
    for i in range(2 * per):
        leaving(i).wait()
    scaled.wait()


def project_kernel(place_ref, slab_ref, hm_ref, lm_ref, ho_ref, lo_ref, *refs):
    out_ref = refs[-1]
    core, rows = place_ref[0], hm_ref.shape[0]
    a, b = slab_ref[part(core, rows), :], slab_ref[part(1 - core, rows), :]
    total = (dot_tn(a, hm_ref[...]) + dot_tn(b, ho_ref[...])) + (
        dot_tn(a, lm_ref[...]) + dot_tn(b, lo_ref[...])
    )
    out_ref[...] = total.astype(BF16)


def image_kernel(in_any, u_any, out_ref, in_ref, u_ref, sems):
    copies = [
        pltpu.make_async_copy(in_any, in_ref, sems.at[0]),
        pltpu.make_async_copy(u_any, u_ref, sems.at[1]),
    ]
    for copy in copies:
        copy.start()
    for copy in copies:
        copy.wait()
    total = in_ref[0].astype(F32)
    for i in range(1, in_ref.shape[0]):
        total = total + in_ref[i].astype(F32)
    high = total.astype(BF16)
    low = (total - high.astype(F32)).astype(BF16)
    out_ref[...] = dot_nn(high, u_ref[0]) + (dot_nn(high, u_ref[1]) + dot_nn(low, u_ref[0]))


def body(slab, sketch):
    core, row = lax.axis_index(C), lax.axis_index(Y)
    place = jnp.stack([core, row]).astype(jnp.int32)
    tokens, columns = slab.shape[0], sketch.shape[1]
    half, block, strip = tokens // 2, tokens // 8, columns // 4

    def partial(which):
        tile = 256
        first = lambda i, place: (place[0] * (half // tile) + i, 0)
        return pl.pallas_call(
            partial_kernel,
            out_shape=struct((half, columns), F32),
            grid_spec=pltpu.PrefetchScalarGridSpec(
                num_scalar_prefetch=1,
                grid=(half // tile,),
                in_specs=[
                    pl.BlockSpec((tile, slab.shape[1]), first),
                    pl.BlockSpec(sketch.shape, lambda i, place: (0, 0)),
                ],
                out_specs=pl.BlockSpec((tile, columns), lambda i, place: (i, 0)),
            ),
            compiler_params=pltpu.CompilerParams(vmem_limit_bytes=16 << 20),
            cost_estimate=pl.CostEstimate(
                flops=2 * half * slab.shape[1] * columns,
                bytes_accessed=2 * half * slab.shape[1] + 4 * half * columns,
                transcendentals=0,
            ),
            name="partial",
        )(jnp.reshape(which, (1,)).astype(jnp.int32), slab, sketch)

    halves = slab.reshape(2, half, slab.shape[1])
    theirs = from_partner(dot_nn(block_of(halves, 1 - core), sketch))
    pair_sum = (partial(core) + theirs).reshape(4, block, columns)
    power = jnp.clip(jnp.floor(jnp.log2(jnp.max(jnp.abs(pair_sum)))), 16.0 - 8 * LEVEL, 40.0)
    lift = jnp.exp2(LEVEL - power)
    tail = tail_of(power, columns)
    own, top = block_of(pair_sum, row), tail
    for s in range(1, 4):
        values = (block_of(pair_sum, (row + s) % 4) * lift).astype(F16)
        got = shifted(jnp.concatenate([values, tail]), Y, s)
        own, top = own + unpacked(got), jnp.maximum(top, got[block:])
    top = jnp.where(lax.broadcasted_iota(jnp.int32, top.shape, 0) < 2, top * 2, top)
    message = jnp.concatenate([(own / unit_of(top)).astype(F16), top])
    pieces = [split(unpacked(message))]
    pieces += [split(unpacked(shifted(message, Y, s))) for s in range(1, 4)]

    pair = struct((half, columns), BF16)
    slice_of = struct((strip // 2, columns), F32)
    high_mine, low_mine, kept, given = pl.pallas_call(
        share_kernel,
        out_shape=(pair, pair, slice_of, slice_of),
        in_specs=[SMEM] + [VMEM] * 8,
        out_specs=(VMEM,) * 4,
        scratch_shapes=[pltpu.VMEM((strip, columns), F32)],
        compiler_params=pltpu.CompilerParams(vmem_limit_bytes=16 << 20),
        name="share",
    )(place, *[p[0] for p in pieces], *[p[1] for p in pieces])
    strip_sum = kept + from_partner(given)
    high_mine, low_mine, strip_sum = lax.optimization_barrier((high_mine, low_mine, strip_sum))
    high_other, low_other = from_partner(high_mine), from_partner(low_mine)

    features = slab.shape[1]
    tile = 256

    def project(first, images):
        steps = features // tile // 2
        whole = pl.BlockSpec((half, columns), lambda i: (0, 0))
        return pl.pallas_call(
            project_kernel,
            out_shape=struct((features, columns), BF16),
            grid=(steps,),
            in_specs=[SMEM, pl.BlockSpec((tokens, tile), lambda i: (0, first * steps + i))]
            + [whole] * 4
            + [ANY] * len(images),
            out_specs=pl.BlockSpec((tile, columns), lambda i: (first * steps + i, 0)),
            input_output_aliases={6: 0} if images else {},
            compiler_params=pltpu.CompilerParams(vmem_limit_bytes=ROOMY),
            cost_estimate=pl.CostEstimate(
                flops=2 * tokens * features * columns,
                bytes_accessed=tokens * (features + 4 * columns) + features * columns,
                transcendentals=0,
            ),
        )(place, slab, high_mine, low_mine, high_other, low_other, *images)

    arrived = exchange(strip_sum.reshape(8, -1, columns), Z)
    images = project(0, ())
    arrived, images = lax.optimization_barrier((arrived, images))
    summed = arrived.sum(axis=0)
    summed = (summed + flipped(summed, X, 1)) + (flipped(summed, X, 2) + flipped(summed, X, 3))
    done = exchange(jnp.broadcast_to(summed[None], (8, *summed.shape)), Z)
    images = project(1, (images,))
    done, images = lax.optimization_barrier((done, images))
    done = done.reshape(-1, columns)

    strips = [done]
    for s in range(1, 4):
        strips.append(shifted(done, Y, s))
    others = [from_partner(s) for s in strips]
    image = exchange(images.reshape(32, -1, columns), TOK)

    token_count = tokens * lax.axis_size(TOK)
    q_basis, r_scaled, upper = pl.pallas_call(
        functools.partial(basis_kernel, 1.0 / math.sqrt(token_count)),
        out_shape=(
            struct((tokens, columns), BF16),
            struct((columns, columns), F32),
            struct((2, columns, columns), BF16),
        ),
        in_specs=[SMEM] + [ANY] * 12,
        out_specs=(ANY, ANY, VMEM),
        scratch_shapes=[pltpu.VMEM((columns, columns), F32)] * 3
        + [
            pltpu.VMEM((4, half, columns), BF16),
            pltpu.VMEM((8, tokens // 8, columns), BF16),
            pltpu.SemaphoreType.DMA((8,)),
            pltpu.SemaphoreType.DMA((4,)),
            pltpu.SemaphoreType.DMA,
            pltpu.SemaphoreType.DMA((8,)),
        ],
        compiler_params=pltpu.CompilerParams(vmem_limit_bytes=51 << 20),
        cost_estimate=pl.CostEstimate(
            flops=20 * tokens * columns * columns,
            bytes_accessed=16 * tokens * columns,
            transcendentals=0,
        ),
        name="basis",
    )(place, *strips, *others, high_mine, low_mine, high_other, low_other)
    projected = pl.pallas_call(
        image_kernel,
        out_shape=struct((image.shape[1], columns), F32),
        in_specs=[ANY] * 2,
        out_specs=VMEM,
        scratch_shapes=[
            pltpu.VMEM(image.shape, BF16),
            pltpu.VMEM((2, columns, columns), BF16),
            pltpu.SemaphoreType.DMA((2,)),
        ],
        compiler_params=pltpu.CompilerParams(vmem_limit_bytes=12 << 20),
        name="image",
    )(image, upper)
    return (q_basis, r_scaled, projected)


def solution(mesh):
    split_mesh = Mesh(mesh.devices.reshape(4, 8, 4, 2), (X, Z, Y, C))
    in_specs = (P(TOK, (Y, C)), P((Y, C), None))
    out_specs = (P(TOK, None), P(), P((Y, C, X, Z), None))
    return jax.shard_map(body, mesh=split_mesh, in_specs=in_specs, out_specs=out_specs, check_vma=False)
```
